32 devices in a mesh: grp: 8 (over z, x), ep: 4 (over y, core).
Axes of the slice: x: 2, y: 2, z: 4, core: 2. Of those that a mesh axis runs over, the one named last changes fastest.
Arguments:
- out_grad: bfloat16 [256, 4096], P('grp', 'ep'), may hold values from -6 to 6
- expert_ids: int32 [256, 8], P('grp'), may hold values from 0 to 15, as said below
- router_logits: float32 [256, 16], P('grp'), may hold values from -5 to 5
- router_weight: bfloat16 [16, 4096], P(None, 'ep'), may hold values from -0.09375 to 0.09375
- expert_weight: bfloat16 [16, 4096, 1024], P('grp', 'ep'), may hold values from -0.1875 to 0.1875
- hidden_saved: bfloat16 [8, 512, 1024], P('grp'), may hold values from -6 to 6
Outputs:
- weight_grad: bfloat16 [16, 4096, 1024], P('grp', 'ep')
- hidden_grad: bfloat16 [8, 512, 1024], P('grp', 'ep')
- input_grad: bfloat16 [256, 4096], P('grp', 'ep')
The draws below stay inside these ranges and needn't reach their ends.
Inputs may be any that keep to these rules, and one draw needn't show every extreme that they name: `expert_ids`: each row names 8 different experts, lying in at most 4 of the 4 groups of 4 consecutive experts. In each aligned block of 32 rows no expert is named by more than 32 rows, and some expert is named by exactly 32.
All inputs are finite; a program needn't handle non-finite values.
Results may differ from the reference program's by a relative error of at most 0.02.
Values may be sent and summed in bfloat16 or wider, within the bound.
A program may use at most 64 MiB of HBM per device.

```python
import jax
import jax.numpy as jnp
from jax import lax

D = 4096
FF = 1024
EXP_GRP = 2
TOPG = 4
TOPK = 8
EXPERTS = 16
GROUPS = 4
GROUP_EXP = 4
PICK = 2
ROWS_GRP = 32
TOKENS = 256
USERS = 32
CAP = 32
SLOTS = 512
N_GRP = 8
N_EP = 4


def draw_expert_ids(key, part):
    group_scores = jax.random.randint(jax.random.fold_in(key, 101), (N_GRP, GROUPS), 0, 1 << 20) * GROUPS + jnp.arange(GROUPS, dtype=jnp.int32)[None, :]
    group_order = jnp.argsort(group_scores, axis=1).astype(jnp.int32)
    user_scores = jax.random.randint(jax.random.fold_in(key, 202), (N_GRP, GROUPS, USERS), 0, 1 << 20) * USERS + jnp.arange(USERS, dtype=jnp.int32)[None, None, :]
    user_order = jnp.argsort(user_scores, axis=2).astype(jnp.int32)
    member_scores = jax.random.randint(jax.random.fold_in(key, 303), (N_GRP, GROUPS, GROUP_EXP), 0, 1 << 20) * GROUP_EXP + jnp.arange(GROUP_EXP, dtype=jnp.int32)[None, None, :]
    member_order = jnp.argsort(member_scores, axis=2).astype(jnp.int32)
    ticket = TOPG * jnp.arange(ROWS_GRP, dtype=jnp.int32)[:, None] + jnp.arange(TOPG, dtype=jnp.int32)[None, :]
    position = ticket % GROUPS
    cycle_index = ticket // GROUPS
    blocks = jnp.arange(N_GRP, dtype=jnp.int32)[:, None, None]
    group_id = group_order[blocks, position[None, :, :]]
    user_slot = user_order[blocks, position[None, :, :], cycle_index[None, :, :]]
    pick_index = user_slot[:, :, :, None] + USERS * jnp.arange(PICK, dtype=jnp.int32)[None, None, None, :]
    member_rank = jnp.where(pick_index < CAP, 0, 1 + (pick_index - CAP) % (GROUP_EXP - 1))
    member = member_order[blocks[:, :, :, None], position[None, :, :, None], member_rank]
    experts = group_id[:, :, :, None] * GROUP_EXP + member
    return experts.reshape(TOKENS, TOPK).astype(jnp.int32)


def level_of(stream_key, extent, shards, low, top_value):
    loudness = 1.0
    for dim, blocks in shards:
        draws = jax.random.uniform(jax.random.fold_in(jax.random.fold_in(stream_key, 6), dim), (blocks,), jnp.float32, low / len(shards), top_value / len(shards))
        loudness = loudness * jnp.repeat(jnp.exp(draws), extent[dim] // blocks).reshape((-1,) + (1,) * (len(extent) - 1 - dim))
    return loudness


def bell_draw(key, shape, scale, reach, pieces=(), kind=jnp.bfloat16):
    entries = scale * jax.random.normal(key, shape, jnp.float32)
    if pieces:
        entries = entries * level_of(key, shape, pieces, -0.22, 0.18)
    return jnp.clip(entries, -reach, reach).astype(kind)


def setup_inputs(seed: int = 0) -> dict:
    key_list = jax.random.split(jax.random.key(seed), 7)
    return {
        "out_grad": bell_draw(key_list[0], (TOKENS, D), 1.0, 6.0, ((0, 8), (1, 4))),
        "expert_ids": draw_expert_ids(jax.random.fold_in(key_list[6], 71), 0),
        "router_logits": bell_draw(key_list[2], (TOKENS, EXPERTS), 1.0, 5.0, ((0, 8),), jnp.float32),
        "router_weight": bell_draw(key_list[3], (EXPERTS, D), D ** -0.5, 0.09375, ((1, 4),)),
        "expert_weight": bell_draw(key_list[4], (EXPERTS, D, FF), FF ** -0.5, 0.1875, ((0, 8), (1, 4))),
        "hidden_saved": bell_draw(key_list[5], (N_GRP, SLOTS, FF), 1.0, 6.0, ((0, 8),)),
    }


route_scale = 2.5


def slot_places(expert_ids):
    pair_rows = expert_ids.reshape(N_GRP, ROWS_GRP * TOPK)
    onehot = (pair_rows[:, :, None] == jnp.arange(EXPERTS, dtype=jnp.int32)[None, None, :]).astype(jnp.int32)
    pair_ranks = jnp.sum((jnp.cumsum(onehot, axis=1) - 1) * onehot, axis=2)
    source_block = jnp.arange(N_GRP, dtype=jnp.int32)[:, None]
    within = ((pair_rows % EXP_GRP) * N_GRP + source_block) * CAP + pair_ranks
    return ((pair_rows // EXP_GRP) * SLOTS + within).reshape(TOKENS * TOPK).astype(jnp.int32)


def reference(out_grad, expert_ids, router_logits, router_weight, expert_weight, hidden_saved):
    sig = jax.nn.sigmoid(router_logits.astype(jnp.float32))
    chosen = jnp.take_along_axis(sig, expert_ids, axis=1)
    route_probs = route_scale * chosen / jnp.sum(chosen, axis=1, keepdims=True)
    places = slot_places(expert_ids)
    pair_token = (jnp.arange(TOKENS * TOPK, dtype=jnp.int32) // TOPK).astype(jnp.int32)
    token_of_slot = jnp.zeros((N_GRP * SLOTS,), jnp.int32).at[places].set(pair_token)
    used_slot = jnp.zeros((N_GRP * SLOTS,), jnp.int32).at[places].set(jnp.ones((TOKENS * TOPK,), jnp.int32))
    slot_prob = jnp.zeros((N_GRP * SLOTS,), jnp.float32).at[places].set(route_probs.reshape(TOKENS * TOPK)).astype(jnp.bfloat16)
    span = N_GRP * CAP
    width = D // N_EP

    def owner_work(items):
        token_index, used_flag, prob_row, saved_rows, weights = items
        slot_rows = jnp.where(used_flag[:, None] > 0, out_grad[token_index], jnp.zeros((), jnp.bfloat16))
        grouped = slot_rows.reshape(EXP_GRP, span, N_EP, width).astype(jnp.float32)
        split_weights = weights.reshape(EXP_GRP, N_EP, width, FF).astype(jnp.float32)
        partial_sums = jnp.einsum("lmkd,lkdf->lkmf", grouped, split_weights)
        rounded = lax.optimization_barrier(partial_sums.astype(jnp.bfloat16)).astype(jnp.float32)
        summed = jnp.sum(rounded, axis=1).reshape(SLOTS, FF)
        prob_value = prob_row.astype(jnp.float32)
        hidden_grad = (prob_value[:, None] * summed).astype(jnp.bfloat16)
        slot_score = jnp.sum(saved_rows.astype(jnp.float32) * summed, axis=1)
        scaled_rows = (prob_value[:, None] * slot_rows.astype(jnp.float32)).astype(jnp.bfloat16)
        weight_grad = jnp.einsum(
            "lmd,lmf->ldf",
            scaled_rows.reshape(EXP_GRP, span, D).astype(jnp.float32),
            saved_rows.reshape(EXP_GRP, span, FF).astype(jnp.float32),
        ).astype(jnp.bfloat16)
        return weight_grad, hidden_grad, slot_score

    weight_grad, hidden_grad, slot_score = lax.map(
        owner_work,
        (
            token_of_slot.reshape(N_GRP, SLOTS),
            used_slot.reshape(N_GRP, SLOTS),
            slot_prob.reshape(N_GRP, SLOTS),
            hidden_saved,
            expert_weight.reshape(N_GRP, EXP_GRP, D, FF),
        ),
    )
    pair_score = slot_score.reshape(N_GRP * SLOTS)[places].reshape(TOKENS, TOPK)
    weighted_mean = jnp.sum(route_probs * pair_score, axis=1, keepdims=True) / route_scale
    logit_terms = route_probs * (1.0 - chosen) * (pair_score - weighted_mean)
    picked = expert_ids[:, :, None] == jnp.arange(EXPERTS, dtype=jnp.int32)[None, None, :]
    router_grad = jnp.sum(jnp.where(picked, logit_terms[:, :, None], jnp.zeros((), jnp.float32)), axis=1).astype(jnp.bfloat16)
    input_grad = jnp.dot(router_grad, router_weight, preferred_element_type=jnp.float32).astype(jnp.bfloat16)
    return weight_grad.reshape(EXPERTS, D, FF), hidden_grad, input_grad
```

```python
import jax
import jax.numpy as jnp
from jax import lax
from jax.experimental import pallas as pl
from jax.experimental.pallas import tpu as pltpu
from jax.sharding import PartitionSpec as P

route_scale = 2.5


def body(out_grad, expert_ids, router_logits, router_weight, expert_weight, hidden_saved):
    group_rows, features = out_grad.shape
    top_count = expert_ids.shape[1]
    experts = router_logits.shape[1]
    group_count = lax.axis_size("grp")
    local_experts = expert_weight.shape[0]
    hidden_width = expert_weight.shape[2]
    slot_count = hidden_saved.shape[1]
    capacity = slot_count // (local_experts * group_count)
    expert_span = group_count * capacity
    pair_count = group_rows * top_count
    sig_values = jax.nn.sigmoid(router_logits)
    picked = expert_ids[:, :, None] == jnp.arange(experts, dtype=jnp.int32)[None, None, :]
    chosen = jnp.sum(jnp.where(picked, sig_values[:, None, :], 0.0), axis=2)
    route_probs = route_scale * chosen / jnp.sum(chosen, axis=1, keepdims=True)
    flat_ids = expert_ids.reshape(pair_count)
    onehot = picked.reshape(pair_count, experts).astype(jnp.int32)
    pair_ranks = jnp.sum((jnp.cumsum(onehot, axis=0) - 1) * onehot, axis=1)
    slot_place = (
        flat_ids % local_experts * group_count + flat_ids // local_experts
    ) * capacity + pair_ranks
    slot_match = slot_place[None, :] == jnp.arange(slot_count, dtype=jnp.int32)[:, None]
    token_pick = jnp.sum(
        slot_match.reshape(slot_count, group_rows, top_count).astype(jnp.float32), axis=2
    ).astype(jnp.bfloat16)
    send_rows = jnp.dot(token_pick, out_grad, preferred_element_type=jnp.float32).astype(
        jnp.bfloat16
    )
    send_prob = jnp.sum(
        jnp.where(slot_match, route_probs.reshape(1, pair_count), 0.0), axis=1
    ).astype(jnp.bfloat16)
    got_rows, got_prob = (
        lax.all_to_all(
            send_rows.reshape(local_experts, group_count, capacity, features),
            "grp",
            split_axis=1,
            concat_axis=1,
            tiled=True,
        ),
        lax.all_to_all(
            send_prob.reshape(local_experts, group_count, capacity),
            "grp",
            split_axis=1,
            concat_axis=1,
            tiled=True,
        ),
    )
    slot_grads = got_rows.reshape(local_experts, expert_span, features)
    prob_rows = got_prob.reshape(local_experts, expert_span).astype(jnp.float32)
    saved_rows = hidden_saved.reshape(local_experts, expert_span, hidden_width)
    scaled_rows = (prob_rows[:, :, None] * slot_grads.astype(jnp.float32)).astype(jnp.bfloat16)
    weight_grad = jnp.einsum(
        "lmd,lmf->ldf", scaled_rows, saved_rows, preferred_element_type=jnp.float32
    ).astype(jnp.bfloat16)
    owner_index = lax.axis_index("ep")
    share_rows = slot_count // lax.axis_size("ep")
    flat_prob = prob_rows.reshape(slot_count)
    flat_saved = hidden_saved.reshape(slot_count, hidden_width)
    partial_term = jnp.einsum(
        "lmd,ldf->lmf", slot_grads, expert_weight, preferred_element_type=jnp.float32
    ).reshape(slot_count, hidden_width)
    rounded_term = lax.optimization_barrier(partial_term.astype(jnp.bfloat16)).astype(jnp.float32)
    partial_score = jnp.sum(flat_saved.astype(jnp.float32) * rounded_term, axis=1)
    moved_scores = lax.all_to_all(
        partial_score.reshape(local_experts, group_count, capacity),
        "grp",
        split_axis=1,
        concat_axis=1,
        tiled=True,
    )
    returned = lax.psum(moved_scores, "ep")
    summed = lax.psum_scatter(
        partial_term.astype(jnp.bfloat16), "ep", scatter_dimension=0, tiled=True
    ).astype(jnp.float32)
    own_prob = lax.dynamic_slice_in_dim(flat_prob, owner_index * share_rows, share_rows, 0)
    hidden_grad = (own_prob[:, None] * summed).astype(jnp.bfloat16)[None]
    pair_score = jnp.sum(
        jnp.where(slot_match, returned.reshape(slot_count, 1), 0.0), axis=0
    ).reshape(group_rows, top_count)
    weighted_mean = jnp.sum(route_probs * pair_score, axis=1, keepdims=True) / route_scale
    logit_terms = route_probs * (1.0 - chosen) * (pair_score - weighted_mean)
    router_grad = jnp.sum(jnp.where(picked, logit_terms[:, :, None], 0.0), axis=1).astype(
        jnp.bfloat16
    )
    input_grad = jnp.dot(router_grad, router_weight, preferred_element_type=jnp.float32).astype(
        jnp.bfloat16
    )
    return (weight_grad, hidden_grad, input_grad)


MESH = pl.DeviceIdType.MESH


def fused_kernel(
    ids_ref, logits_ref, grad_ref, rw_ref, w_hbm, saved_hbm,
    scaled_ref, hidden_ref, input_ref,
    w_ref, saved_ref, rows_all, probs_all, probs_own, slot_ref, slot_rows, prob_col, part,
    recv_a, send_b, recv_b, score_own, score_recv, score_rows,
    w_sem, saved_sem, rows_send, rows_recv, probs_send, probs_recv,
    a_send, a_recv, b_send, b_recv, sc_send, sc_recv,
):
    groups = lax.axis_size("grp")
    parts = lax.axis_size("ep")
    chips = parts // 2
    g = lax.axis_index("grp")
    k = lax.axis_index("ep")
    chip, core = k // 2, k % 2
    rows, features = grad_ref.shape
    experts = logits_ref.shape[0]
    top = ids_ref.shape[0]
    local, span, width = part.shape
    half_groups = groups // 2
    half_tokens = half_groups * rows
    tokens = groups * rows
    share = span // 2
    capacity = span // groups
    f32, bf16 = jnp.float32, jnp.bfloat16

    barrier = pltpu.get_barrier_semaphore()
    for dg in range(groups):
        for dk in range(parts):
            if dg or dk:
                pl.semaphore_signal(
                    barrier, inc=1,
                    device_id=(lax.rem(g + dg, groups), lax.rem(k + dk, parts)),
                    device_id_type=MESH,
                )
    w_copies = [
        pltpu.make_async_copy(w_hbm.at[i], w_ref.at[i], w_sem.at[i]) for i in range(local)
    ]
    for copy in w_copies:
        copy.start()
    saved_copy = pltpu.make_async_copy(saved_hbm, saved_ref, saved_sem)
    saved_copy.start()

    sig = 1.0 / (1.0 + jnp.exp(-logits_ref[...]))
    ids = ids_ref[...]
    expert_iota = lax.broadcasted_iota(jnp.int32, (experts, rows), 0)
    named = ids[0:1, :] == expert_iota
    for i in range(1, top):
        named = named | (ids[i : i + 1, :] == expert_iota)
    probs = route_scale * sig / jnp.sum(jnp.where(named, sig, 0.0), axis=0, keepdims=True)
    probs = jnp.where(named, probs, 0.0)
    lane_off = lax.rem(g, half_groups) * rows
    place = (
        lax.broadcasted_iota(jnp.int32, (rows, half_tokens), 1)
        == lax.broadcasted_iota(jnp.int32, (rows, half_tokens), 0) + lane_off
    )
    placed = jnp.dot(
        probs.astype(bf16), place.astype(f32).astype(bf16), preferred_element_type=f32
    ).astype(bf16)
    probs_own[...] = placed
    probs_all[g] = placed
    rows_all[pl.ds(pl.multiple_of(g * rows, rows), rows), :] = grad_ref[...]

    pl.semaphore_wait(barrier, groups * parts - 1)

    parity, pos = lax.rem(g, 2), g // 2
    mate = g + 1 - 2 * parity

    def block(b):
        return rows_all.at[pl.ds(pl.multiple_of(b * rows, rows), rows), :]

    def rows_copy(src, b, to, sem):
        return pltpu.make_async_remote_copy(
            src_ref=src, dst_ref=block(b), send_sem=rows_send.at[sem], recv_sem=rows_recv.at[b],
            device_id=(to, k), device_id_type=MESH,
        )

    sends = []
    peers = [lax.rem(pos + j, half_groups) * 2 + parity for j in range(1, half_groups)]
    for j in range(1, groups):
        to = lax.rem(g + j, groups)
        copy = pltpu.make_async_remote_copy(
            src_ref=probs_own, dst_ref=probs_all.at[g],
            send_sem=probs_send.at[j - 1], recv_sem=probs_recv.at[g],
            device_id=(to, k), device_id_type=MESH,
        )
        copy.start()
        sends.append(copy)
    for n, to in enumerate([*peers, mate]):
        copy = rows_copy(grad_ref, g, to, n)
        copy.start()
        sends.append(copy)
    for n, peer in enumerate(peers):
        rows_copy(block(peer), peer, g, 0).wait_recv()
        copy = rows_copy(block(peer), peer, mate, half_groups + n)
        copy.start()
        sends.append(copy)

    for j in range(1, groups):
        b = lax.rem(g + j, groups)
        pltpu.make_async_remote_copy(
            src_ref=probs_own, dst_ref=probs_all.at[b],
            send_sem=probs_send.at[0], recv_sem=probs_recv.at[b],
            device_id=(g, k), device_id_type=MESH,
        ).wait_recv()
    pick = (
        lax.broadcasted_iota(jnp.int32, (8, experts), 1)
        == lax.broadcasted_iota(jnp.int32, (8, experts), 0) + g * local
    ) & (lax.broadcasted_iota(jnp.int32, (8, experts), 0) < local)
    pick = pick.astype(f32).astype(bf16)
    halves = []
    for h in range(2):
        total = probs_all[h * half_groups].astype(f32)
        for b in range(1, half_groups):
            total = total + probs_all[h * half_groups + b].astype(f32)
        halves.append(jnp.dot(pick, total.astype(bf16), preferred_element_type=f32))
    lane = lax.broadcasted_iota(jnp.int32, (half_tokens, half_tokens), 1)
    before = lax.broadcasted_iota(jnp.int32, (half_tokens, half_tokens), 0)
    earlier = (before < lane) & (before // rows == lane // rows)
    earlier = earlier.astype(f32).astype(bf16)
    half_block = lax.broadcasted_iota(jnp.int32, (8, half_tokens), 1) // rows
    for h in range(2):
        used = halves[h] > 0.0
        rank = jnp.dot(used.astype(f32).astype(bf16), earlier, preferred_element_type=f32)
        slot = (half_block + h * half_groups) * capacity + rank.astype(jnp.int32)
        slot_ref[h] = jnp.where(used, slot, -1)
    prob_tokens = jnp.concatenate(halves, axis=1)

    def slot_row(l, h):
        table = slot_ref[h]
        mask = lax.broadcasted_iota(jnp.int32, table.shape, 0) == l
        return jnp.sum(jnp.where(mask, table, 0), axis=0, keepdims=True)

    for l in range(local):
        row = jnp.concatenate([slot_row(l, 0), slot_row(l, 1)], axis=1)
        match = lax.broadcasted_iota(jnp.int32, (span, tokens), 0) == row
        prob_col[l] = jnp.sum(
            jnp.where(match, prob_tokens[l : l + 1, :], 0.0), axis=1, keepdims=True
        )

    rows_copy(grad_ref, mate, g, 0).wait_recv()
    for n, peer in enumerate(peers):
        b = peer + 1 - 2 * parity
        rows_copy(grad_ref, b, g, 0).wait_recv()
    for copy in w_copies:
        copy.wait()

    order = [lax.rem(chip + 1 + i, chips) for i in range(chips)]

    def a_copy(l, half, to):
        return pltpu.make_async_remote_copy(
            src_ref=part.at[l, pl.ds(pl.multiple_of(half * share, share), share), :],
            dst_ref=recv_a.at[l], send_sem=a_send.at[l], recv_sem=a_recv.at[l],
            device_id=(g, to), device_id_type=MESH,
        )

    def b_copy(l):
        return pltpu.make_async_remote_copy(
            src_ref=send_b.at[l], dst_ref=recv_b.at[chip],
            send_sem=b_send.at[l], recv_sem=b_recv.at[chip],
            device_id=(g, l * 2 + core), device_id_type=MESH,
        )

    partner = k + 1 - 2 * core
    step = min(width, 256)
    for l in order:
        row = jnp.concatenate([slot_row(l, 0), slot_row(l, 1)], axis=1)
        match = lax.broadcasted_iota(jnp.int32, (span, tokens), 0) == row
        slot_rows[l] = jnp.dot(
            match.astype(f32).astype(bf16), rows_all[...], preferred_element_type=f32
        ).astype(bf16)
        for n in range(0, width, step):
            part[l, :, n : n + step] = jnp.dot(
                slot_rows[l], w_ref[l, :, n : n + step], preferred_element_type=f32
            ).astype(bf16)
        copy = a_copy(l, 1 - core, partner)
        copy.start()
        sends.append(copy)

    saved_copy.wait()
    kept = pl.ds(pl.multiple_of(core * share, share), share)
    for i, l in enumerate(order):
        a_copy(l, 1 - core, partner).wait_recv()
        both = part[l, kept, :].astype(f32) + recv_a[l].astype(f32)
        send_b[l] = both.astype(bf16)
        if i < chips - 1:
            copy = b_copy(l)
            copy.start()
            sends.append(copy)
        start = pl.multiple_of(l * span + core * share, share)
        score = jnp.sum(
            saved_ref[pl.ds(start, share), :].astype(f32) * both, axis=1, keepdims=True
        )
        match = (
            lax.broadcasted_iota(jnp.int32, (share, half_tokens), 0) + core * share
            == slot_row(l, core)
        )
        score_own[pl.ds(l, 1), :] = jnp.sum(jnp.where(match, score, 0.0), axis=0, keepdims=True)

    def score_copy(b, to, sem, y, o):
        return pltpu.make_async_remote_copy(
            src_ref=score_own, dst_ref=score_recv.at[y, o],
            send_sem=sc_send.at[sem], recv_sem=sc_recv.at[y * groups + o],
            device_id=(b, to), device_id_type=MESH,
        )

    for j in range(half_groups):
        b = core * half_groups + j
        for dk in range(parts):
            copy = score_copy(b, lax.rem(k + dk, parts), j * parts + dk, chip, g)
            if dk:
                copy.start()
            else:
                pl.when(b != g)(copy.start)

    my_half = g // half_groups

    @pl.when(my_half == core)
    def _():
        score_recv[chip, g] = score_own[...]

    for l in range(local):
        scaled_ref[l] = (prob_col[l] * slot_rows[l].astype(f32)).astype(bf16)

    for i in range(chips - 1):
        source = order[i]
        pltpu.make_async_remote_copy(
            src_ref=send_b.at[0], dst_ref=recv_b.at[source],
            send_sem=b_send.at[0], recv_sem=b_recv.at[source],
            device_id=(g, k), device_id_type=MESH,
        ).wait_recv()
    total = send_b[chip].astype(f32)
    for i in range(chips - 1):
        total = total + recv_b[order[i]].astype(f32)
    hidden_ref[...] = (prob_col[chip, kept, :] * total).astype(bf16)

    for y in range(chips):
        for o in range(groups):
            wait = score_copy(g, k, 0, y, o).wait_recv
            pl.when((o != g) | (y != chip) | (my_half != core))(wait)
    for o in range(groups):
        value = score_recv[0, o]
        for y in range(1, chips):
            value = value + score_recv[y, o]
        score_rows[o * local : (o + 1) * local, :] = value
    take = (
        lax.broadcasted_iota(jnp.int32, (half_tokens, rows), 0)
        == lax.broadcasted_iota(jnp.int32, (half_tokens, rows), 1) + lane_off
    )
    pair = jnp.dot(
        score_rows[...], take.astype(f32), preferred_element_type=f32,
        precision=lax.Precision.HIGHEST,
    )
    mean = jnp.sum(probs * pair, axis=0, keepdims=True) / route_scale
    terms = jnp.where(named, probs * (1.0 - sig) * (pair - mean), 0.0).astype(bf16)
    eye = (
        lax.broadcasted_iota(jnp.int32, (rows, rows), 0)
        == lax.broadcasted_iota(jnp.int32, (rows, rows), 1)
    )
    turned = lax.dot_general(
        eye.astype(f32).astype(bf16), terms, (((1,), (1,)), ((), ())), preferred_element_type=f32
    ).astype(bf16)
    input_ref[...] = jnp.dot(turned, rw_ref[...], preferred_element_type=f32).astype(bf16)

    for copy in sends:
        copy.wait_send()
    for j in range(half_groups):
        b = core * half_groups + j
        for dk in range(parts):
            wait = score_copy(b, lax.rem(k + dk, parts), j * parts + dk, chip, g).wait_send
            if dk:
                wait()
            else:
                pl.when(b != g)(wait)


def fused(out_grad, expert_ids, router_logits, router_weight, expert_weight, hidden_saved):
    groups, parts = lax.axis_size("grp"), lax.axis_size("ep")
    rows, features = out_grad.shape
    experts = router_logits.shape[1]
    local, _, width = expert_weight.shape
    slots = hidden_saved.shape[1]
    span = slots // local
    half_tokens = groups // 2 * rows
    share = span // 2
    chips = parts // 2
    f32, bf16 = jnp.float32, jnp.bfloat16
    vmem = pl.BlockSpec(memory_space=pltpu.VMEM)
    anyspace = pl.BlockSpec(memory_space=pl.ANY)
    dma = pltpu.SemaphoreType.DMA
    scaled, hidden, input_grad = pl.pallas_call(
        fused_kernel,
        out_shape=(
            jax.ShapeDtypeStruct((local, span, features), bf16),
            jax.ShapeDtypeStruct((share, width), bf16),
            jax.ShapeDtypeStruct((rows, features), bf16),
        ),
        in_specs=[vmem, vmem, vmem, vmem, anyspace, anyspace],
        out_specs=(vmem, vmem, vmem),
        scratch_shapes=[
            pltpu.VMEM((local, features, width), bf16),
            pltpu.VMEM((slots, width), bf16),
            pltpu.VMEM((groups * rows, features), bf16),
            pltpu.VMEM((groups, experts, half_tokens), bf16),
            pltpu.VMEM((experts, half_tokens), bf16),
            pltpu.VMEM((2, 8, half_tokens), jnp.int32),
            pltpu.VMEM((local, span, features), bf16),
            pltpu.VMEM((local, span, 1), f32),
            pltpu.VMEM((local, span, width), bf16),
            pltpu.VMEM((local, share, width), bf16),
            pltpu.VMEM((local, share, width), bf16),
            pltpu.VMEM((chips, share, width), bf16),
            pltpu.VMEM((local, half_tokens), f32),
            pltpu.VMEM((chips, groups, local, half_tokens), f32),
            pltpu.VMEM((experts, half_tokens), f32),
            dma((local,)), dma, dma((groups - 1,)), dma((groups,)),
            dma((groups - 1,)), dma((groups,)),
            dma((local,)), dma((local,)), dma((local,)), dma((chips,)),
            dma((groups // 2 * parts,)), dma((chips * groups,)),
        ],
        compiler_params=pltpu.CompilerParams(
            collective_id=0, has_side_effects=True, vmem_limit_bytes=40 * 1024 * 1024
        ),
    )(
        expert_ids.T, router_logits.T, out_grad, router_weight, expert_weight,
        hidden_saved.reshape(slots, width),
    )
    saved_rows = hidden_saved.reshape(local, span, width)
    weight_grad = jnp.einsum(
        "lmd,lmf->ldf", scaled, saved_rows, preferred_element_type=f32
    ).astype(bf16)
    return weight_grad, hidden[None], input_grad


def choose(*args):
    out_grad, _, _, _, expert_weight, hidden_saved = args
    groups, parts = lax.axis_size("grp"), lax.axis_size("ep")
    rows, local = out_grad.shape[0], expert_weight.shape[0]
    slots_for_one = hidden_saved.shape[1] // groups
    lanes = groups // 2 * rows
    if parts == 2 * local and groups % 2 == 0 and rows <= slots_for_one and lanes % 128 == 0:
        return fused(*args)
    return body(*args)


def solution(mesh):
    in_specs = (
        P("grp", "ep"),
        P("grp", None),
        P("grp", None),
        P(None, "ep"),
        P("grp", "ep", None),
        P("grp", None, None),
    )
    out_specs = (P("grp", "ep", None), P("grp", "ep", None), P("grp", "ep"))
    return jax.shard_map(choose, mesh=mesh, in_specs=in_specs, out_specs=out_specs, check_vma=False)
```

```python
import jax
import jax.numpy as jnp
from jax import lax
from jax.experimental import pallas as pl
from jax.experimental.pallas import tpu as pltpu
from jax.sharding import PartitionSpec as P

route_scale = 2.5


def body(out_grad, expert_ids, router_logits, router_weight, expert_weight, hidden_saved):
    group_rows, features = out_grad.shape
    top_count = expert_ids.shape[1]
    experts = router_logits.shape[1]
    group_count = lax.axis_size("grp")
    local_experts = expert_weight.shape[0]
    hidden_width = expert_weight.shape[2]
    slot_count = hidden_saved.shape[1]
    capacity = slot_count // (local_experts * group_count)
    expert_span = group_count * capacity
    pair_count = group_rows * top_count
    sig_values = jax.nn.sigmoid(router_logits)
    picked = expert_ids[:, :, None] == jnp.arange(experts, dtype=jnp.int32)[None, None, :]
    chosen = jnp.sum(jnp.where(picked, sig_values[:, None, :], 0.0), axis=2)
    route_probs = route_scale * chosen / jnp.sum(chosen, axis=1, keepdims=True)
    flat_ids = expert_ids.reshape(pair_count)
    onehot = picked.reshape(pair_count, experts).astype(jnp.int32)
    pair_ranks = jnp.sum((jnp.cumsum(onehot, axis=0) - 1) * onehot, axis=1)
    slot_place = (
        flat_ids % local_experts * group_count + flat_ids // local_experts
    ) * capacity + pair_ranks
    slot_match = slot_place[None, :] == jnp.arange(slot_count, dtype=jnp.int32)[:, None]
    token_pick = jnp.sum(
        slot_match.reshape(slot_count, group_rows, top_count).astype(jnp.float32), axis=2
    ).astype(jnp.bfloat16)
    send_rows = jnp.dot(token_pick, out_grad, preferred_element_type=jnp.float32).astype(
        jnp.bfloat16
    )
    send_prob = jnp.sum(
        jnp.where(slot_match, route_probs.reshape(1, pair_count), 0.0), axis=1
    ).astype(jnp.bfloat16)
    got_rows, got_prob = (
        lax.all_to_all(
            send_rows.reshape(local_experts, group_count, capacity, features),
            "grp",
            split_axis=1,
            concat_axis=1,
            tiled=True,
        ),
        lax.all_to_all(
            send_prob.reshape(local_experts, group_count, capacity),
            "grp",
            split_axis=1,
            concat_axis=1,
            tiled=True,
        ),
    )
    slot_grads = got_rows.reshape(local_experts, expert_span, features)
    prob_rows = got_prob.reshape(local_experts, expert_span).astype(jnp.float32)
    saved_rows = hidden_saved.reshape(local_experts, expert_span, hidden_width)
    scaled_rows = (prob_rows[:, :, None] * slot_grads.astype(jnp.float32)).astype(jnp.bfloat16)
    weight_grad = jnp.einsum(
        "lmd,lmf->ldf", scaled_rows, saved_rows, preferred_element_type=jnp.float32
    ).astype(jnp.bfloat16)
    owner_index = lax.axis_index("ep")
    share_rows = slot_count // lax.axis_size("ep")
    flat_prob = prob_rows.reshape(slot_count)
    flat_saved = hidden_saved.reshape(slot_count, hidden_width)
    partial_term = jnp.einsum(
        "lmd,ldf->lmf", slot_grads, expert_weight, preferred_element_type=jnp.float32
    ).reshape(slot_count, hidden_width)
    rounded_term = lax.optimization_barrier(partial_term.astype(jnp.bfloat16)).astype(jnp.float32)
    partial_score = jnp.sum(flat_saved.astype(jnp.float32) * rounded_term, axis=1)
    moved_scores = lax.all_to_all(
        partial_score.reshape(local_experts, group_count, capacity),
        "grp",
        split_axis=1,
        concat_axis=1,
        tiled=True,
    )
    returned = lax.psum(moved_scores, "ep")
    summed = lax.psum_scatter(
        partial_term.astype(jnp.bfloat16), "ep", scatter_dimension=0, tiled=True
    ).astype(jnp.float32)
    own_prob = lax.dynamic_slice_in_dim(flat_prob, owner_index * share_rows, share_rows, 0)
    hidden_grad = (own_prob[:, None] * summed).astype(jnp.bfloat16)[None]
    pair_score = jnp.sum(
        jnp.where(slot_match, returned.reshape(slot_count, 1), 0.0), axis=0
    ).reshape(group_rows, top_count)
    weighted_mean = jnp.sum(route_probs * pair_score, axis=1, keepdims=True) / route_scale
    logit_terms = route_probs * (1.0 - chosen) * (pair_score - weighted_mean)
    router_grad = jnp.sum(jnp.where(picked, logit_terms[:, :, None], 0.0), axis=1).astype(
        jnp.bfloat16
    )
    input_grad = jnp.dot(router_grad, router_weight, preferred_element_type=jnp.float32).astype(
        jnp.bfloat16
    )
    return (weight_grad, hidden_grad, input_grad)


MESH = pl.DeviceIdType.MESH


def fused_kernel(
    ids_hbm, logits_hbm, grad_hbm, rw_hbm, w_hbm, saved_hbm,
    wg_ref, hidden_ref, input_ref,
    ids_ref, logits_ref, grad_ref, rw_ref, in_sem, scaled, w_ref, saved_ref, rows_all, probs_all, probs_own, slot_ref, slot_rows, prob_col, part,
    recv_a, send_b, recv_b, score_own, score_recv, score_rows,
    w_sem, saved_sem, rows_send, rows_recv, probs_send, probs_recv,
    a_send, a_recv, b_send, b_recv, sc_send, sc_recv,
):
    groups = lax.axis_size("grp")
    parts = lax.axis_size("ep")
    chips = parts // 2
    g = lax.axis_index("grp")
    k = lax.axis_index("ep")
    chip, core = k // 2, k % 2
    rows, features = grad_ref.shape
    experts = logits_ref.shape[0]
    top = ids_ref.shape[0]
    local, span, width = part.shape
    half_groups = groups // 2
    half_tokens = half_groups * rows
    tokens = groups * rows
    share = span // 2
    capacity = span // groups
    f32, bf16 = jnp.float32, jnp.bfloat16

    barrier = pltpu.get_barrier_semaphore()
    for dg in range(groups):
        for dk in range(parts):
            if dg or dk:
                pl.semaphore_signal(
                    barrier, inc=1,
                    device_id=(lax.rem(g + dg, groups), lax.rem(k + dk, parts)),
                    device_id_type=MESH,
                )
    small = [
        pltpu.make_async_copy(src, dst, in_sem.at[i])
        for i, (src, dst) in enumerate(
            [(ids_hbm, ids_ref), (logits_hbm, logits_ref), (grad_hbm, grad_ref), (rw_hbm, rw_ref)]
        )
    ]
    for copy in small:
        copy.start()
    w_copies = [
        pltpu.make_async_copy(w_hbm.at[i], w_ref.at[i], w_sem.at[i]) for i in range(local)
    ]
    for copy in w_copies:
        copy.start()
    saved_copy = pltpu.make_async_copy(saved_hbm, saved_ref, saved_sem)
    saved_copy.start()

    small[0].wait()
    small[1].wait()
    sig = 1.0 / (1.0 + jnp.exp(-logits_ref[...]))
    ids = ids_ref[...]
    expert_iota = lax.broadcasted_iota(jnp.int32, (experts, rows), 0)
    named = ids[0:1, :] == expert_iota
    for i in range(1, top):
        named = named | (ids[i : i + 1, :] == expert_iota)
    probs = route_scale * sig / jnp.sum(jnp.where(named, sig, 0.0), axis=0, keepdims=True)
    probs = jnp.where(named, probs, 0.0)
    lane_off = lax.rem(g, half_groups) * rows
    place = (
        lax.broadcasted_iota(jnp.int32, (rows, half_tokens), 1)
        == lax.broadcasted_iota(jnp.int32, (rows, half_tokens), 0) + lane_off
    )
    placed = jnp.dot(
        probs.astype(bf16), place.astype(f32).astype(bf16), preferred_element_type=f32
    ).astype(bf16)
    probs_own[...] = placed
    probs_all[g] = placed
    small[2].wait()
    rows_all[pl.ds(pl.multiple_of(g * rows, rows), rows), :] = grad_ref[...]

    pl.semaphore_wait(barrier, groups * parts - 1)

    def across(index, mask):
        bit = 1
        while bit <= mask:
            if mask & bit:
                index = index + bit - 2 * bit * lax.rem(index // bit, 2)
            bit *= 2
        return index

    def block(b):
        return rows_all.at[pl.ds(pl.multiple_of(b * rows, rows), rows), :]

    def rows_copy(src, b, to, sem):
        return pltpu.make_async_remote_copy(
            src_ref=src, dst_ref=block(b), send_sem=rows_send.at[sem], recv_sem=rows_recv.at[b],
            device_id=(to, k), device_id_type=MESH,
        )

    sends = []
    for j in range(1, groups):
        to = lax.rem(g + j, groups)
        copy = pltpu.make_async_remote_copy(
            src_ref=probs_own, dst_ref=probs_all.at[g],
            send_sem=probs_send.at[j - 1], recv_sem=probs_recv.at[g],
            device_id=(to, k), device_id_type=MESH,
        )
        copy.start()
        sends.append(copy)

    def spread(src, mask):
        stride = groups // 2 if mask == 0 else (mask & -mask) // 2
        while stride >= 1:
            copy = rows_copy(src, across(g, mask), across(g, stride), mask | stride)
            copy.start()
            sends.append(copy)
            stride //= 2

    def arrive(mask):
        b = across(g, mask)
        rows_copy(block(b), b, g, 0).wait_recv()
        spread(block(b), mask)

    spread(grad_ref, 0)
    arrive(2)
    arrive(half_groups)

    for j in range(1, groups):
        b = lax.rem(g + j, groups)
        pltpu.make_async_remote_copy(
            src_ref=probs_own, dst_ref=probs_all.at[b],
            send_sem=probs_send.at[0], recv_sem=probs_recv.at[b],
            device_id=(g, k), device_id_type=MESH,
        ).wait_recv()
    pick = (
        lax.broadcasted_iota(jnp.int32, (8, experts), 1)
        == lax.broadcasted_iota(jnp.int32, (8, experts), 0) + g * local
    ) & (lax.broadcasted_iota(jnp.int32, (8, experts), 0) < local)
    pick = pick.astype(f32).astype(bf16)
    halves = []
    for h in range(2):
        total = probs_all[h * half_groups].astype(f32)
        for b in range(1, half_groups):
            total = total + probs_all[h * half_groups + b].astype(f32)
        halves.append(jnp.dot(pick, total.astype(bf16), preferred_element_type=f32))
    lane = lax.broadcasted_iota(jnp.int32, (half_tokens, half_tokens), 1)
    before = lax.broadcasted_iota(jnp.int32, (half_tokens, half_tokens), 0)
    earlier = (before < lane) & (before // rows == lane // rows)
    earlier = earlier.astype(f32).astype(bf16)
    half_block = lax.broadcasted_iota(jnp.int32, (8, half_tokens), 1) // rows
    for h in range(2):
        used = halves[h] > 0.0
        rank = jnp.dot(used.astype(f32).astype(bf16), earlier, preferred_element_type=f32)
        slot = (half_block + h * half_groups) * capacity + rank.astype(jnp.int32)
        slot_ref[h] = jnp.where(used, slot, -1)
    prob_tokens = jnp.concatenate(halves, axis=1)

    def slot_row(l, h):
        table = slot_ref[h]
        mask = lax.broadcasted_iota(jnp.int32, table.shape, 0) == l
        return jnp.sum(jnp.where(mask, table, 0), axis=0, keepdims=True)

    for l in range(local):
        row = jnp.concatenate([slot_row(l, 0), slot_row(l, 1)], axis=1)
        match = lax.broadcasted_iota(jnp.int32, (span, tokens), 0) == row
        prob_col[l] = jnp.sum(
            jnp.where(match, prob_tokens[l : l + 1, :], 0.0), axis=1, keepdims=True
        )

    for copy in w_copies:
        copy.wait()

    order = [lax.rem(chip + 1 + i, chips) for i in range(chips)]

    def a_copy(l, half, to):
        return pltpu.make_async_remote_copy(
            src_ref=part.at[l, pl.ds(pl.multiple_of(half * share, share), share), :],
            dst_ref=recv_a.at[l], send_sem=a_send.at[l], recv_sem=a_recv.at[l],
            device_id=(g, to), device_id_type=MESH,
        )

    def b_copy(l):
        return pltpu.make_async_remote_copy(
            src_ref=send_b.at[l], dst_ref=recv_b.at[chip],
            send_sem=b_send.at[l], recv_sem=b_recv.at[chip],
            device_id=(g, l * 2 + core), device_id_type=MESH,
        )

    partner = k + 1 - 2 * core
    step = min(width, 256)
    near = g // half_groups
    far = 1 - near
    kept = pl.ds(pl.multiple_of(core * share, share), share)

    def multiply(l, half):
        own = pl.ds(pl.multiple_of(half * share, share), share)
        match = (
            lax.broadcasted_iota(jnp.int32, (share, half_tokens), 0) + half * share
            == slot_row(l, half)
        )
        gathered = rows_all[pl.ds(pl.multiple_of(half * half_tokens, half_tokens), half_tokens), :]
        slot_rows[l, own, :] = jnp.dot(
            match.astype(f32).astype(bf16), gathered, preferred_element_type=f32
        ).astype(bf16)
        for n in range(0, width, step):
            part[l, own, n : n + step] = jnp.dot(
                slot_rows[l, own, :], w_ref[l, :, n : n + step], preferred_element_type=f32
            ).astype(bf16)

        @pl.when(half != core)
        def _():
            a_copy(l, 1 - core, partner).start()

    def combine(i):
        l = order[i]
        a_copy(l, 1 - core, partner).wait_recv()
        both = part[l, kept, :].astype(f32) + recv_a[l].astype(f32)
        send_b[l] = both.astype(bf16)
        if i < chips - 1:
            b_copy(l).start()
        start = pl.multiple_of(l * span + core * share, share)
        score = jnp.sum(
            saved_ref[pl.ds(start, share), :].astype(f32) * both, axis=1, keepdims=True
        )
        match = (
            lax.broadcasted_iota(jnp.int32, (share, half_tokens), 0) + core * share
            == slot_row(l, core)
        )
        score_own[pl.ds(l, 1), :] = jnp.sum(jnp.where(match, score, 0.0), axis=0, keepdims=True)

    late = [m for m in range(half_groups + 1, groups)]
    forwarders = [m for m in late if m % 2 == 0]
    for mask in range(1, half_groups):
        if mask != 2:
            arrive(mask)
    multiply(order[0], near)
    for mask in forwarders:
        arrive(mask)
    for i in range(1, chips):
        multiply(order[i], near)
    saved_copy.wait()

    @pl.when(near == core)
    def _():
        for i in range(chips - 1):
            combine(i)

    for mask in late:
        if mask % 2:
            arrive(mask)
    for i in range(chips):
        multiply(order[i], far)

    @pl.when(near != core)
    def _():
        for i in range(chips - 1):
            combine(i)

    combine(chips - 1)

    def score_copy(b, to, sem, y, o):
        return pltpu.make_async_remote_copy(
            src_ref=score_own, dst_ref=score_recv.at[y, o],
            send_sem=sc_send.at[sem], recv_sem=sc_recv.at[y * groups + o],
            device_id=(b, to), device_id_type=MESH,
        )

    for j in range(half_groups):
        b = core * half_groups + j
        for dk in range(parts):
            copy = score_copy(b, lax.rem(k + dk, parts), j * parts + dk, chip, g)
            if dk:
                copy.start()
            else:
                pl.when(b != g)(copy.start)

    my_half = g // half_groups

    @pl.when(my_half == core)
    def _():
        score_recv[chip, g] = score_own[...]

    for l in range(local):
        scaled[l] = (prob_col[l] * slot_rows[l].astype(f32)).astype(bf16)
        for n in range(0, features, min(features, 256)):
            wg_ref[l, n : n + min(features, 256), :] = lax.dot_general(
                scaled[l, :, n : n + min(features, 256)],
                saved_ref[l * span : (l + 1) * span, :],
                (((0,), (0,)), ((), ())),
                preferred_element_type=f32,
            ).astype(bf16)

    for i in range(chips - 1):
        source = order[i]
        pltpu.make_async_remote_copy(
            src_ref=send_b.at[0], dst_ref=recv_b.at[source],
            send_sem=b_send.at[0], recv_sem=b_recv.at[source],
            device_id=(g, k), device_id_type=MESH,
        ).wait_recv()
    total = send_b[chip].astype(f32)
    for i in range(chips - 1):
        total = total + recv_b[order[i]].astype(f32)
    hidden_ref[...] = (prob_col[chip, kept, :] * total).astype(bf16)

    for y in range(chips):
        for o in range(groups):
            wait = score_copy(g, k, 0, y, o).wait_recv
            pl.when((o != g) | (y != chip) | (my_half != core))(wait)
    for o in range(groups):
        value = score_recv[0, o]
        for y in range(1, chips):
            value = value + score_recv[y, o]
        score_rows[o * local : (o + 1) * local, :] = value
    take = (
        lax.broadcasted_iota(jnp.int32, (half_tokens, rows), 0)
        == lax.broadcasted_iota(jnp.int32, (half_tokens, rows), 1) + lane_off
    )
    pair = jnp.dot(
        score_rows[...], take.astype(f32), preferred_element_type=f32,
        precision=lax.Precision.HIGHEST,
    )
    mean = jnp.sum(probs * pair, axis=0, keepdims=True) / route_scale
    terms = jnp.where(named, probs * (1.0 - sig) * (pair - mean), 0.0).astype(bf16)
    eye = (
        lax.broadcasted_iota(jnp.int32, (rows, rows), 0)
        == lax.broadcasted_iota(jnp.int32, (rows, rows), 1)
    )
    turned = lax.dot_general(
        eye.astype(f32).astype(bf16), terms, (((1,), (1,)), ((), ())), preferred_element_type=f32
    ).astype(bf16)
    small[3].wait()
    input_ref[...] = jnp.dot(turned, rw_ref[...], preferred_element_type=f32).astype(bf16)

    for copy in sends:
        copy.wait_send()
    for l in order:
        a_copy(l, 1 - core, partner).wait_send()
    for l in order[:-1]:
        b_copy(l).wait_send()
    for j in range(half_groups):
        b = core * half_groups + j
        for dk in range(parts):
            wait = score_copy(b, lax.rem(k + dk, parts), j * parts + dk, chip, g).wait_send
            if dk:
                wait()
            else:
                pl.when(b != g)(wait)


def store_kernel(a, b, c, a_out, b_out, c_out, sem):
    copies = [
        pltpu.make_async_copy(src, dst, sem.at[i])
        for i, (src, dst) in enumerate([(a, a_out), (b, b_out), (c, c_out)])
    ]
    for copy in copies:
        copy.start()
    for copy in copies:
        copy.wait()


def fused(out_grad, expert_ids, router_logits, router_weight, expert_weight, hidden_saved):
    groups, parts = lax.axis_size("grp"), lax.axis_size("ep")
    rows, features = out_grad.shape
    experts = router_logits.shape[1]
    local, _, width = expert_weight.shape
    slots = hidden_saved.shape[1]
    span = slots // local
    half_tokens = groups // 2 * rows
    share = span // 2
    chips = parts // 2
    f32, bf16 = jnp.float32, jnp.bfloat16
    vmem = pl.BlockSpec(memory_space=pltpu.VMEM)
    hbm = pl.BlockSpec(memory_space=pltpu.HBM)
    dma = pltpu.SemaphoreType.DMA
    weight_grad, hidden, input_grad = pl.pallas_call(
        fused_kernel,
        out_shape=(
            jax.ShapeDtypeStruct((local, features, width), bf16),
            jax.ShapeDtypeStruct((share, width), bf16),
            jax.ShapeDtypeStruct((rows, features), bf16),
        ),
        in_specs=[hbm] * 6,
        out_specs=(vmem, vmem, vmem),
        scratch_shapes=[
            pltpu.VMEM(expert_ids.shape[::-1], jnp.int32),
            pltpu.VMEM(router_logits.shape[::-1], f32),
            pltpu.VMEM(out_grad.shape, bf16),
            pltpu.VMEM(router_weight.shape, bf16),
            dma((4,)),
            pltpu.VMEM((local, span, features), bf16),
            pltpu.VMEM((local, features, width), bf16),
            pltpu.VMEM((slots, width), bf16),
            pltpu.VMEM((groups * rows, features), bf16),
            pltpu.VMEM((groups, experts, half_tokens), bf16),
            pltpu.VMEM((experts, half_tokens), bf16),
            pltpu.VMEM((2, 8, half_tokens), jnp.int32),
            pltpu.VMEM((local, span, features), bf16),
            pltpu.VMEM((local, span, 1), f32),
            pltpu.VMEM((local, span, width), bf16),
            pltpu.VMEM((local, share, width), bf16),
            pltpu.VMEM((local, share, width), bf16),
            pltpu.VMEM((chips, share, width), bf16),
            pltpu.VMEM((local, half_tokens), f32),
            pltpu.VMEM((chips, groups, local, half_tokens), f32),
            pltpu.VMEM((experts, half_tokens), f32),
            dma((local,)), dma, dma((groups,)), dma((groups,)),
            dma((groups - 1,)), dma((groups,)),
            dma((local,)), dma((local,)), dma((local,)), dma((chips,)),
            dma((groups // 2 * parts,)), dma((chips * groups,)),
        ],
        compiler_params=pltpu.CompilerParams(
            collective_id=0, has_side_effects=True, vmem_limit_bytes=40 * 1024 * 1024
        ),
    )(*[
        pltpu.with_memory_space_constraint(x, pltpu.HBM)
        for x in (
            expert_ids.T, router_logits.T, out_grad, router_weight, expert_weight,
            hidden_saved.reshape(slots, width),
        )
    ])
    results = (weight_grad, hidden, input_grad)
    weight_grad, hidden, input_grad = pl.pallas_call(
        store_kernel,
        out_shape=tuple(jax.ShapeDtypeStruct(r.shape, r.dtype) for r in results),
        in_specs=[vmem] * 3,
        out_specs=(hbm,) * 3,
        scratch_shapes=[dma((3,))],
        compiler_params=pltpu.CompilerParams(vmem_limit_bytes=1024 * 1024),
    )(*results)
    return weight_grad, hidden[None], input_grad


def choose(*args):
    out_grad, _, _, _, expert_weight, hidden_saved = args
    groups, parts = lax.axis_size("grp"), lax.axis_size("ep")
    rows, local = out_grad.shape[0], expert_weight.shape[0]
    slots_for_one = hidden_saved.shape[1] // groups
    lanes = groups // 2 * rows
    if parts == 2 * local and groups >= 4 and groups & (groups - 1) == 0 and rows <= slots_for_one and lanes % 128 == 0:
        return fused(*args)
    return body(*args)


def solution(mesh):
    in_specs = (
        P("grp", "ep"),
        P("grp", None),
        P("grp", None),
        P(None, "ep"),
        P("grp", "ep", None),
        P("grp", None, None),
    )
    out_specs = (P("grp", "ep", None), P("grp", "ep", None), P("grp", "ep"))
    return jax.shard_map(choose, mesh=mesh, in_specs=in_specs, out_specs=out_specs, check_vma=False)
```

```python
import jax
import jax.numpy as jnp
from jax import lax
from jax.experimental import pallas as pl
from jax.experimental.pallas import tpu as pltpu
from jax.sharding import PartitionSpec as P

route_scale = 2.5


def body(out_grad, expert_ids, router_logits, router_weight, expert_weight, hidden_saved):
    group_rows, features = out_grad.shape
    top_count = expert_ids.shape[1]
    experts = router_logits.shape[1]
    group_count = lax.axis_size("grp")
    local_experts = expert_weight.shape[0]
    hidden_width = expert_weight.shape[2]
    slot_count = hidden_saved.shape[1]
    capacity = slot_count // (local_experts * group_count)
    expert_span = group_count * capacity
    pair_count = group_rows * top_count
    sig_values = jax.nn.sigmoid(router_logits)
    picked = expert_ids[:, :, None] == jnp.arange(experts, dtype=jnp.int32)[None, None, :]
    chosen = jnp.sum(jnp.where(picked, sig_values[:, None, :], 0.0), axis=2)
    route_probs = route_scale * chosen / jnp.sum(chosen, axis=1, keepdims=True)
    flat_ids = expert_ids.reshape(pair_count)
    onehot = picked.reshape(pair_count, experts).astype(jnp.int32)
    pair_ranks = jnp.sum((jnp.cumsum(onehot, axis=0) - 1) * onehot, axis=1)
    slot_place = (
        flat_ids % local_experts * group_count + flat_ids // local_experts
    ) * capacity + pair_ranks
    slot_match = slot_place[None, :] == jnp.arange(slot_count, dtype=jnp.int32)[:, None]
    token_pick = jnp.sum(
        slot_match.reshape(slot_count, group_rows, top_count).astype(jnp.float32), axis=2
    ).astype(jnp.bfloat16)
    send_rows = jnp.dot(token_pick, out_grad, preferred_element_type=jnp.float32).astype(
        jnp.bfloat16
    )
    send_prob = jnp.sum(
        jnp.where(slot_match, route_probs.reshape(1, pair_count), 0.0), axis=1
    ).astype(jnp.bfloat16)
    got_rows, got_prob = (
        lax.all_to_all(
            send_rows.reshape(local_experts, group_count, capacity, features),
            "grp",
            split_axis=1,
            concat_axis=1,
            tiled=True,
        ),
        lax.all_to_all(
            send_prob.reshape(local_experts, group_count, capacity),
            "grp",
            split_axis=1,
            concat_axis=1,
            tiled=True,
        ),
    )
    slot_grads = got_rows.reshape(local_experts, expert_span, features)
    prob_rows = got_prob.reshape(local_experts, expert_span).astype(jnp.float32)
    saved_rows = hidden_saved.reshape(local_experts, expert_span, hidden_width)
    scaled_rows = (prob_rows[:, :, None] * slot_grads.astype(jnp.float32)).astype(jnp.bfloat16)
    weight_grad = jnp.einsum(
        "lmd,lmf->ldf", scaled_rows, saved_rows, preferred_element_type=jnp.float32
    ).astype(jnp.bfloat16)
    owner_index = lax.axis_index("ep")
    share_rows = slot_count // lax.axis_size("ep")
    flat_prob = prob_rows.reshape(slot_count)
    flat_saved = hidden_saved.reshape(slot_count, hidden_width)
    partial_term = jnp.einsum(
        "lmd,ldf->lmf", slot_grads, expert_weight, preferred_element_type=jnp.float32
    ).reshape(slot_count, hidden_width)
    rounded_term = lax.optimization_barrier(partial_term.astype(jnp.bfloat16)).astype(jnp.float32)
    partial_score = jnp.sum(flat_saved.astype(jnp.float32) * rounded_term, axis=1)
    moved_scores = lax.all_to_all(
        partial_score.reshape(local_experts, group_count, capacity),
        "grp",
        split_axis=1,
        concat_axis=1,
        tiled=True,
    )
    returned = lax.psum(moved_scores, "ep")
    summed = lax.psum_scatter(
        partial_term.astype(jnp.bfloat16), "ep", scatter_dimension=0, tiled=True
    ).astype(jnp.float32)
    own_prob = lax.dynamic_slice_in_dim(flat_prob, owner_index * share_rows, share_rows, 0)
    hidden_grad = (own_prob[:, None] * summed).astype(jnp.bfloat16)[None]
    pair_score = jnp.sum(
        jnp.where(slot_match, returned.reshape(slot_count, 1), 0.0), axis=0
    ).reshape(group_rows, top_count)
    weighted_mean = jnp.sum(route_probs * pair_score, axis=1, keepdims=True) / route_scale
    logit_terms = route_probs * (1.0 - chosen) * (pair_score - weighted_mean)
    router_grad = jnp.sum(jnp.where(picked, logit_terms[:, :, None], 0.0), axis=1).astype(
        jnp.bfloat16
    )
    input_grad = jnp.dot(router_grad, router_weight, preferred_element_type=jnp.float32).astype(
        jnp.bfloat16
    )
    return (weight_grad, hidden_grad, input_grad)


MESH = pl.DeviceIdType.MESH


def fused_kernel(
    ids_hbm, logits_hbm, grad_hbm, rw_hbm, w_hbm, saved_hbm,
    wg_ref, hidden_ref, input_ref,
    ids_ref, logits_ref, grad_ref, rw_ref, in_sem, scaled, w_ref, saved_ref, rows_all, probs_all, probs_own, slot_ref, slot_rows, prob_col, part,
    recv_a, send_b, recv_b, score_own, score_recv, score_rows,
    w_sem, saved_sem, rows_send, rows_recv, probs_send, probs_recv,
    a_send, a_recv, b_send, b_recv, sc_send, sc_recv,
):
    groups = lax.axis_size("grp")
    parts = lax.axis_size("ep")
    chips = parts // 2
    g = lax.axis_index("grp")
    k = lax.axis_index("ep")
    chip, core = k // 2, k % 2
    rows, features = grad_ref.shape
    experts = logits_ref.shape[0]
    top = ids_ref.shape[0]
    local, span, width = part.shape
    half_groups = groups // 2
    half_tokens = half_groups * rows
    tokens = groups * rows
    share = span // 2
    capacity = span // groups
    f32, bf16 = jnp.float32, jnp.bfloat16

    barrier = pltpu.get_barrier_semaphore()
    for dg in range(groups):
        for dk in range(parts):
            if dg or dk:
                pl.semaphore_signal(
                    barrier, inc=1,
                    device_id=(lax.rem(g + dg, groups), lax.rem(k + dk, parts)),
                    device_id_type=MESH,
                )
    small = [
        pltpu.make_async_copy(src, dst, in_sem.at[i])
        for i, (src, dst) in enumerate(
            [(ids_hbm, ids_ref), (logits_hbm, logits_ref), (grad_hbm, grad_ref), (rw_hbm, rw_ref)]
        )
    ]
    for copy in small:
        copy.start()
    w_copies = [
        pltpu.make_async_copy(w_hbm.at[i], w_ref.at[i], w_sem.at[i]) for i in range(local)
    ]
    for copy in w_copies:
        copy.start()
    saved_copy = pltpu.make_async_copy(saved_hbm, saved_ref, saved_sem)
    saved_copy.start()

    small[0].wait()
    small[1].wait()
    sig = 1.0 / (1.0 + jnp.exp(-logits_ref[...]))
    ids = ids_ref[...]
    expert_iota = lax.broadcasted_iota(jnp.int32, (experts, rows), 0)
    named = ids[0:1, :] == expert_iota
    for i in range(1, top):
        named = named | (ids[i : i + 1, :] == expert_iota)
    probs = route_scale * sig / jnp.sum(jnp.where(named, sig, 0.0), axis=0, keepdims=True)
    probs = jnp.where(named, probs, 0.0)
    lane_off = lax.rem(g, half_groups) * rows
    place = (
        lax.broadcasted_iota(jnp.int32, (rows, half_tokens), 1)
        == lax.broadcasted_iota(jnp.int32, (rows, half_tokens), 0) + lane_off
    )
    placed = jnp.dot(
        probs.astype(bf16), place.astype(f32).astype(bf16), preferred_element_type=f32
    ).astype(bf16)
    probs_own[...] = placed
    probs_all[g] = placed
    small[2].wait()
    rows_all[pl.ds(pl.multiple_of(g * rows, rows), rows), :] = grad_ref[...]

    pl.semaphore_wait(barrier, groups * parts - 1)

    def across(index, mask):
        bit = 1
        while bit <= mask:
            if mask & bit:
                index = index + bit - 2 * bit * lax.rem(index // bit, 2)
            bit *= 2
        return index

    pieces = rows_recv.shape[1]
    piece_rows = rows // pieces

    def block(b, piece):
        start = pl.multiple_of(b * rows + piece * piece_rows, piece_rows)
        return rows_all.at[pl.ds(start, piece_rows), :]

    def own_piece(piece):
        return grad_ref.at[pl.ds(piece * piece_rows, piece_rows), :]

    def rows_copy(src, b, to, sem, piece):
        return pltpu.make_async_remote_copy(
            src_ref=src, dst_ref=block(b, piece),
            send_sem=rows_send.at[sem, piece], recv_sem=rows_recv.at[b, piece],
            device_id=(to, k), device_id_type=MESH,
        )

    sends = []
    for j in range(1, groups):
        to = lax.rem(g + j, groups)
        copy = pltpu.make_async_remote_copy(
            src_ref=probs_own, dst_ref=probs_all.at[g],
            send_sem=probs_send.at[j - 1], recv_sem=probs_recv.at[g],
            device_id=(to, k), device_id_type=MESH,
        )
        copy.start()
        sends.append(copy)

    def spread(src, mask, piece):
        stride = groups // 2 if mask == 0 else (mask & -mask) // 2
        while stride >= 1:
            copy = rows_copy(src, across(g, mask), across(g, stride), mask | stride, piece)
            copy.start()
            sends.append(copy)
            stride //= 2

    def arrive(mask, piece):
        b = across(g, mask)
        rows_copy(block(b, piece), b, g, 0, piece).wait_recv()
        spread(block(b, piece), mask, piece)

    for piece in range(pieces):
        spread(own_piece(piece), 0, piece)
    for mask in (2, half_groups):
        for piece in range(pieces):
            arrive(mask, piece)

    for j in range(1, groups):
        b = lax.rem(g + j, groups)
        pltpu.make_async_remote_copy(
            src_ref=probs_own, dst_ref=probs_all.at[b],
            send_sem=probs_send.at[0], recv_sem=probs_recv.at[b],
            device_id=(g, k), device_id_type=MESH,
        ).wait_recv()
    pick = (
        lax.broadcasted_iota(jnp.int32, (8, experts), 1)
        == lax.broadcasted_iota(jnp.int32, (8, experts), 0) + g * local
    ) & (lax.broadcasted_iota(jnp.int32, (8, experts), 0) < local)
    pick = pick.astype(f32).astype(bf16)
    halves = []
    for h in range(2):
        total = probs_all[h * half_groups].astype(f32)
        for b in range(1, half_groups):
            total = total + probs_all[h * half_groups + b].astype(f32)
        halves.append(jnp.dot(pick, total.astype(bf16), preferred_element_type=f32))
    lane = lax.broadcasted_iota(jnp.int32, (half_tokens, half_tokens), 1)
    before = lax.broadcasted_iota(jnp.int32, (half_tokens, half_tokens), 0)
    earlier = (before < lane) & (before // rows == lane // rows)
    earlier = earlier.astype(f32).astype(bf16)
    half_block = lax.broadcasted_iota(jnp.int32, (8, half_tokens), 1) // rows
    for h in range(2):
        used = halves[h] > 0.0
        rank = jnp.dot(used.astype(f32).astype(bf16), earlier, preferred_element_type=f32)
        slot = (half_block + h * half_groups) * capacity + rank.astype(jnp.int32)
        slot_ref[h] = jnp.where(used, slot, -1)
    prob_tokens = jnp.concatenate(halves, axis=1)

    def slot_row(l, h):
        table = slot_ref[h]
        mask = lax.broadcasted_iota(jnp.int32, table.shape, 0) == l
        return jnp.sum(jnp.where(mask, table, 0), axis=0, keepdims=True)

    for l in range(local):
        row = jnp.concatenate([slot_row(l, 0), slot_row(l, 1)], axis=1)
        match = lax.broadcasted_iota(jnp.int32, (span, tokens), 0) == row
        prob_col[l] = jnp.sum(
            jnp.where(match, prob_tokens[l : l + 1, :], 0.0), axis=1, keepdims=True
        )

    for copy in w_copies:
        copy.wait()

    order = [lax.rem(chip + 1 + i, chips) for i in range(chips)]

    def a_copy(l, half, to):
        return pltpu.make_async_remote_copy(
            src_ref=part.at[l, pl.ds(pl.multiple_of(half * share, share), share), :],
            dst_ref=recv_a.at[l], send_sem=a_send.at[l], recv_sem=a_recv.at[l],
            device_id=(g, to), device_id_type=MESH,
        )

    def b_copy(l):
        return pltpu.make_async_remote_copy(
            src_ref=send_b.at[l], dst_ref=recv_b.at[chip],
            send_sem=b_send.at[l], recv_sem=b_recv.at[chip],
            device_id=(g, l * 2 + core), device_id_type=MESH,
        )

    partner = k + 1 - 2 * core
    step = min(width, 256)
    near = g // half_groups
    far = 1 - near
    kept = pl.ds(pl.multiple_of(core * share, share), share)

    def multiply(l, half):
        own = pl.ds(pl.multiple_of(half * share, share), share)
        match = (
            lax.broadcasted_iota(jnp.int32, (share, half_tokens), 0) + half * share
            == slot_row(l, half)
        )
        gathered = rows_all[pl.ds(pl.multiple_of(half * half_tokens, half_tokens), half_tokens), :]
        slot_rows[l, own, :] = jnp.dot(
            match.astype(f32).astype(bf16), gathered, preferred_element_type=f32
        ).astype(bf16)
        for n in range(0, width, step):
            part[l, own, n : n + step] = jnp.dot(
                slot_rows[l, own, :], w_ref[l, :, n : n + step], preferred_element_type=f32
            ).astype(bf16)

        @pl.when(half != core)
        def _():
            a_copy(l, 1 - core, partner).start()

    def combine(i):
        l = order[i]
        a_copy(l, 1 - core, partner).wait_recv()
        both = part[l, kept, :].astype(f32) + recv_a[l].astype(f32)
        send_b[l] = both.astype(bf16)
        if i < chips - 1:
            b_copy(l).start()
        start = pl.multiple_of(l * span + core * share, share)
        score = jnp.sum(
            saved_ref[pl.ds(start, share), :].astype(f32) * both, axis=1, keepdims=True
        )
        match = (
            lax.broadcasted_iota(jnp.int32, (share, half_tokens), 0) + core * share
            == slot_row(l, core)
        )
        score_own[pl.ds(l, 1), :] = jnp.sum(jnp.where(match, score, 0.0), axis=0, keepdims=True)

    late = [m for m in range(half_groups + 1, groups)]
    forwarders = [m for m in late if m % 2 == 0]
    for mask in range(1, half_groups):
        for piece in range(pieces):
            if mask != 2:
                arrive(mask, piece)
    multiply(order[0], near)
    for mask in forwarders:
        arrive(mask, 0)
    for i in range(1, chips):
        multiply(order[i], near)
    for mask in forwarders:
        for piece in range(1, pieces):
            arrive(mask, piece)
    saved_copy.wait()

    @pl.when(near == core)
    def _():
        for i in range(chips - 1):
            combine(i)

    for mask in late:
        for piece in range(pieces):
            if mask % 2:
                arrive(mask, piece)
    for i in range(chips):
        multiply(order[i], far)

    @pl.when(near != core)
    def _():
        for i in range(chips - 1):
            combine(i)

    combine(chips - 1)

    def score_copy(b, to, sem, y, o):
        return pltpu.make_async_remote_copy(
            src_ref=score_own, dst_ref=score_recv.at[y, o],
            send_sem=sc_send.at[sem], recv_sem=sc_recv.at[y * groups + o],
            device_id=(b, to), device_id_type=MESH,
        )

    for j in range(half_groups):
        b = core * half_groups + j
        for dk in range(parts):
            copy = score_copy(b, lax.rem(k + dk, parts), j * parts + dk, chip, g)
            if dk:
                copy.start()
            else:
                pl.when(b != g)(copy.start)

    my_half = g // half_groups

    @pl.when(my_half == core)
    def _():
        score_recv[chip, g] = score_own[...]

    for l in range(local):
        scaled[l] = (prob_col[l] * slot_rows[l].astype(f32)).astype(bf16)
        for n in range(0, features, min(features, 256)):
            wg_ref[l, n : n + min(features, 256), :] = lax.dot_general(
                scaled[l, :, n : n + min(features, 256)],
                saved_ref[l * span : (l + 1) * span, :],
                (((0,), (0,)), ((), ())),
                preferred_element_type=f32,
            ).astype(bf16)

    for i in range(chips - 1):
        source = order[i]
        pltpu.make_async_remote_copy(
            src_ref=send_b.at[0], dst_ref=recv_b.at[source],
            send_sem=b_send.at[0], recv_sem=b_recv.at[source],
            device_id=(g, k), device_id_type=MESH,
        ).wait_recv()
    total = send_b[chip].astype(f32)
    for i in range(chips - 1):
        total = total + recv_b[order[i]].astype(f32)
    hidden_ref[...] = (prob_col[chip, kept, :] * total).astype(bf16)

    for y in range(chips):
        for o in range(groups):
            wait = score_copy(g, k, 0, y, o).wait_recv
            pl.when((o != g) | (y != chip) | (my_half != core))(wait)
    for o in range(groups):
        value = score_recv[0, o]
        for y in range(1, chips):
            value = value + score_recv[y, o]
        score_rows[o * local : (o + 1) * local, :] = value
    take = (
        lax.broadcasted_iota(jnp.int32, (half_tokens, rows), 0)
        == lax.broadcasted_iota(jnp.int32, (half_tokens, rows), 1) + lane_off
    )
    pair = jnp.dot(
        score_rows[...], take.astype(f32), preferred_element_type=f32,
        precision=lax.Precision.HIGHEST,
    )
    mean = jnp.sum(probs * pair, axis=0, keepdims=True) / route_scale
    terms = jnp.where(named, probs * (1.0 - sig) * (pair - mean), 0.0).astype(bf16)
    eye = (
        lax.broadcasted_iota(jnp.int32, (rows, rows), 0)
        == lax.broadcasted_iota(jnp.int32, (rows, rows), 1)
    )
    turned = lax.dot_general(
        eye.astype(f32).astype(bf16), terms, (((1,), (1,)), ((), ())), preferred_element_type=f32
    ).astype(bf16)
    small[3].wait()
    input_ref[...] = jnp.dot(turned, rw_ref[...], preferred_element_type=f32).astype(bf16)

    for copy in sends:
        copy.wait_send()
    for l in order:
        a_copy(l, 1 - core, partner).wait_send()
    for l in order[:-1]:
        b_copy(l).wait_send()
    for j in range(half_groups):
        b = core * half_groups + j
        for dk in range(parts):
            wait = score_copy(b, lax.rem(k + dk, parts), j * parts + dk, chip, g).wait_send
            if dk:
                wait()
            else:
                pl.when(b != g)(wait)


def store_kernel(a, b, c, a_out, b_out, c_out, sem):
    count, depth, _ = a.shape
    cuts = (sem.shape[0] - 2) // count
    cut = depth // cuts
    copies = [
        pltpu.make_async_copy(b, b_out, sem.at[0]), pltpu.make_async_copy(c, c_out, sem.at[1])
    ]
    for i in range(count):
        for j in range(cuts):
            span = pl.ds(j * cut, cut)
            copies.append(
                pltpu.make_async_copy(
                    a.at[i, span, :], a_out.at[i, span, :], sem.at[2 + i * cuts + j]
                )
            )
    for copy in copies:
        copy.start()
    for copy in copies:
        copy.wait()


def fused(out_grad, expert_ids, router_logits, router_weight, expert_weight, hidden_saved):
    groups, parts = lax.axis_size("grp"), lax.axis_size("ep")
    rows, features = out_grad.shape
    experts = router_logits.shape[1]
    local, _, width = expert_weight.shape
    slots = hidden_saved.shape[1]
    span = slots // local
    half_tokens = groups // 2 * rows
    share = span // 2
    chips = parts // 2
    pieces = 2 if rows % 32 == 0 else 1
    f32, bf16 = jnp.float32, jnp.bfloat16
    vmem = pl.BlockSpec(memory_space=pltpu.VMEM)
    hbm = pl.BlockSpec(memory_space=pltpu.HBM)
    dma = pltpu.SemaphoreType.DMA
    weight_grad, hidden, input_grad = pl.pallas_call(
        fused_kernel,
        out_shape=(
            jax.ShapeDtypeStruct((local, features, width), bf16),
            jax.ShapeDtypeStruct((share, width), bf16),
            jax.ShapeDtypeStruct((rows, features), bf16),
        ),
        in_specs=[hbm] * 6,
        out_specs=(vmem, vmem, vmem),
        scratch_shapes=[
            pltpu.VMEM(expert_ids.shape[::-1], jnp.int32),
            pltpu.VMEM(router_logits.shape[::-1], f32),
            pltpu.VMEM(out_grad.shape, bf16),
            pltpu.VMEM(router_weight.shape, bf16),
            dma((4,)),
            pltpu.VMEM((local, span, features), bf16),
            pltpu.VMEM((local, features, width), bf16),
            pltpu.VMEM((slots, width), bf16),
            pltpu.VMEM((groups * rows, features), bf16),
            pltpu.VMEM((groups, experts, half_tokens), bf16),
            pltpu.VMEM((experts, half_tokens), bf16),
            pltpu.VMEM((2, 8, half_tokens), jnp.int32),
            pltpu.VMEM((local, span, features), bf16),
            pltpu.VMEM((local, span, 1), f32),
            pltpu.VMEM((local, span, width), bf16),
            pltpu.VMEM((local, share, width), bf16),
            pltpu.VMEM((local, share, width), bf16),
            pltpu.VMEM((chips, share, width), bf16),
            pltpu.VMEM((local, half_tokens), f32),
            pltpu.VMEM((chips, groups, local, half_tokens), f32),
            pltpu.VMEM((experts, half_tokens), f32),
            dma((local,)), dma, dma((groups, pieces)), dma((groups, pieces)),
            dma((groups - 1,)), dma((groups,)),
            dma((local,)), dma((local,)), dma((local,)), dma((chips,)),
            dma((groups // 2 * parts,)), dma((chips * groups,)),
        ],
        compiler_params=pltpu.CompilerParams(
            collective_id=0, has_side_effects=True, vmem_limit_bytes=40 * 1024 * 1024
        ),
    )(*[
        pltpu.with_memory_space_constraint(x, pltpu.HBM)
        for x in (
            expert_ids.T, router_logits.T, out_grad, router_weight, expert_weight,
            hidden_saved.reshape(slots, width),
        )
    ])
    results = (weight_grad, hidden, input_grad)
    weight_grad, hidden, input_grad = pl.pallas_call(
        store_kernel,
        out_shape=tuple(jax.ShapeDtypeStruct(r.shape, r.dtype) for r in results),
        in_specs=[vmem] * 3,
        out_specs=(hbm,) * 3,
        scratch_shapes=[dma((2 + 4 * local,))],
        compiler_params=pltpu.CompilerParams(vmem_limit_bytes=1024 * 1024),
    )(*results)
    return weight_grad, hidden[None], input_grad


def choose(*args):
    out_grad, _, _, _, expert_weight, hidden_saved = args
    groups, parts = lax.axis_size("grp"), lax.axis_size("ep")
    rows, local = out_grad.shape[0], expert_weight.shape[0]
    slots_for_one = hidden_saved.shape[1] // groups
    lanes = groups // 2 * rows
    if parts == 2 * local and groups >= 4 and groups & (groups - 1) == 0 and rows <= slots_for_one and lanes % 128 == 0:
        return fused(*args)
    return body(*args)


def solution(mesh):
    in_specs = (
        P("grp", "ep"),
        P("grp", None),
        P("grp", None),
        P(None, "ep"),
        P("grp", "ep", None),
        P("grp", None, None),
    )
    out_specs = (P("grp", "ep", None), P("grp", "ep", None), P("grp", "ep"))
    return jax.shard_map(choose, mesh=mesh, in_specs=in_specs, out_specs=out_specs, check_vma=False)
```
